32 devices in a mesh: south: 2 (over core), east: 4 (over z), down: 2 (over x), ens: 2 (over y).
Axes of the slice: x: 2, y: 2, z: 4, core: 2. Of those that a mesh axis runs over, the one named last changes fastest.
Arguments:
- density: float32 [16, 128, 128, 128], P(('ens', 'south'), 'east', 'down'), parts along dimension 0, may hold values from 0.2 to 1.8
- flow_j: float32 [16, 128, 128, 128], P(('ens', 'south'), 'east', 'down'), parts along dimension 0, may hold values from -0.3 to 0.3
- flow_i: float32 [16, 128, 128, 128], P(('ens', 'south'), 'east', 'down'), parts along dimension 0, may hold values from -0.3 to 0.3
- flow_k: float32 [16, 128, 128, 128], P(('ens', 'south'), 'east', 'down'), parts along dimension 0, may hold values from -0.3 to 0.3
Outputs:
- density_end: float32 [16, 128, 128, 128], P(('ens', 'south'), 'east', 'down'), parts along dimension 0
The draws below stay inside these ranges and needn't reach their ends.
There are 2 independent parts, one for each index of `ens`. The reference program is written for one: setup_inputs(seed, part) draws one part's arguments, and reference() takes and returns one part's arrays. A program takes and returns all parts, laid end to end along the dimension named above; each array names one. Nothing has to cross between parts.
All inputs are finite; a program needn't handle non-finite values.
Results may differ from the reference program's by a relative error of at most 0.00002.
Values sent between devices are 32-bit elements; how exact they have to be, the bound alone decides.
No kernel may reach another device: no remote copies, remote signals or barrier semaphores. Data moves between devices by JAX's collectives and lax.ppermute only.
A program may use at most 192 MiB of HBM per device.

```python
import jax
import jax.numpy as jnp
from jax import lax

GRID_J = 8
GRID_I = 128
GRID_K = 128
SPECIES = 128
STEPS = 3


def levels(own_key, extent, split, low, top_value):
    def one(axis_at, blocks):
        draws = jax.random.uniform(jax.random.fold_in(jax.random.fold_in(own_key, 6), axis_at), (blocks,), jnp.float32, low / len(split), top_value / len(split))
        return jnp.repeat(jnp.exp(draws), extent[axis_at] // blocks).reshape((-1,) + (1,) * (len(extent) - axis_at - 1))

    gain = one(*split[0])
    for cut in split[1:]:
        gain = gain * one(*cut)
    return gain


def setup_inputs(seed: int = 0, part: int = 0) -> dict:
    keys = jax.random.split(jax.random.key(seed), 5)
    part_keys = jax.random.split(jax.random.fold_in(keys[4], part), 5)
    density = jnp.clip(0.2 + 1.5999999 * jax.random.uniform(part_keys[0], (GRID_J, GRID_I, GRID_K, SPECIES), jnp.float32) ** levels(part_keys[0], (GRID_J, GRID_I, GRID_K, SPECIES), ((0, 2), (1, 4), (2, 2)), -0.2, 0.2), 0.2, 1.8)
    flow_j = jnp.clip(jax.random.uniform(part_keys[1], (GRID_J, GRID_I, GRID_K, SPECIES), jnp.float32, -0.3, 0.3) * levels(part_keys[1], (GRID_J, GRID_I, GRID_K, SPECIES), ((0, 2), (1, 4), (2, 2)), -0.4, 0.0), -0.3, 0.3)
    flow_i = jnp.clip(jax.random.uniform(part_keys[2], (GRID_J, GRID_I, GRID_K, SPECIES), jnp.float32, -0.3, 0.3) * levels(part_keys[2], (GRID_J, GRID_I, GRID_K, SPECIES), ((0, 2), (1, 4), (2, 2)), -0.4, 0.0), -0.3, 0.3)
    flow_k = jnp.clip(jax.random.uniform(part_keys[3], (GRID_J, GRID_I, GRID_K, SPECIES), jnp.float32, -0.3, 0.3) * levels(part_keys[3], (GRID_J, GRID_I, GRID_K, SPECIES), ((0, 2), (1, 4), (2, 2)), -0.4, 0.0), -0.3, 0.3)
    return dict(density=density, flow_j=flow_j, flow_i=flow_i, flow_k=flow_k)


def inner_cells(values, dims):
    for dim in dims:
        values = lax.slice_in_dim(values, 1, values.shape[dim] - 1, axis=dim)
    return values


def side_cells(values, dim, start, dims):
    others = [other for other in dims if other != dim]
    values = inner_cells(values, others)
    return lax.slice_in_dim(values, start, start + values.shape[dim] - 2, axis=dim)


def advance(padded, flow_j, flow_i, flow_k):
    middle = inner_cells(padded, (0, 1, 2))
    lower = [side_cells(padded, dim, 0, (0, 1, 2)) for dim in (0, 1, 2)]
    upper = [side_cells(padded, dim, 2, (0, 1, 2)) for dim in (0, 1, 2)]
    slopes = [above - below for above, below in zip(upper, lower)]
    smooth_rate = 0.05
    spread = lower[0] + upper[0] + lower[1] + upper[1] + lower[2] + upper[2] - 6.0 * middle
    return middle - flow_j * slopes[0] - flow_i * slopes[1] - flow_k * slopes[2] + smooth_rate * spread


def reference(density, flow_j, flow_i, flow_k):
    for step in range(STEPS):
        density = advance(jnp.pad(density, ((1, 1), (1, 1), (1, 1), (0, 0)), mode="constant"), flow_j, flow_i, flow_k)
    return density
```

```python
import functools

import jax
import jax.numpy as jnp
from jax import lax
from jax.experimental import pallas as pl
from jax.experimental.pallas import tpu as pltpu
from jax.sharding import PartitionSpec as P

STEPS = 3
AXES = ("south", "east", "down")
RATE = 0.05


def exchange(axis, faces):
    count = lax.axis_size(axis)
    if len(faces) == 1:
        return [lax.ppermute(faces[0], axis, [(0, 1), (1, 0)])]
    up = [(i, i + 1) for i in range(count - 1)]
    first, last = faces
    return [lax.ppermute(last, axis, up), lax.ppermute(first, axis, [(j, i) for i, j in up])]


def main_kernel(d_ref, fj_ref, fi_ref, fk_ref, o_ref):
    nj, ni, nk, _ = d_ref.shape
    row = lax.broadcasted_iota(jnp.int32, d_ref.shape[2:], 0)

    for j in range(nj):

        @pl.loop(0, ni)
        def _(i, j=j):
            m = d_ref[j, i]
            below = jnp.maximum(i - 1, 0)
            above = jnp.minimum(i + 1, ni - 1)
            lo = jnp.where(i > 0, RATE, 0.0)
            hi = jnp.where(i < ni - 1, RATE, 0.0)
            lo1 = jnp.where(i > 0, 1.0, 0.0)
            hi1 = jnp.where(i < ni - 1, 1.0, 0.0)
            im = d_ref[j, below] * lo1
            ip = d_ref[j, above] * hi1
            km = jnp.where(row == 0, 0.0, pltpu.roll(m, 1, 0))
            kp = jnp.where(row == nk - 1, 0.0, pltpu.roll(m, nk - 1, 0))
            total = im + ip + (km + kp)
            out = m - fi_ref[j, i] * (ip - im) - fk_ref[j, i] * (kp - km)
            fj = fj_ref[j, i]
            if j > 0 and j < nj - 1:
                jm, jp = d_ref[j - 1, i], d_ref[j + 1, i]
                total = total + (jm + jp)
                out = out - fj * (jp - jm)
            elif j > 0:
                jm = d_ref[j - 1, i]
                total = total + jm
                out = out + fj * jm
            elif nj > 1:
                jp = d_ref[j + 1, i]
                total = total + jp
                out = out - fj * jp
            o_ref[j, i] = out + RATE * (total - 6.0 * m)


def patch_kernel(counts, emit, *refs):
    d_ref, fj_ref, fi_ref, fk_ref = refs[:4]
    at = 4
    halos = []
    for count in counts:
        size = 1 if count == 2 else 2 if count > 2 else 0
        halos.append(refs[at : at + size])
        at += size
    o_ref = refs[at]
    faces, at = [], at + 1
    if emit:
        for halo in halos:
            faces.append(refs[at : at + len(halo)])
            at += len(halo)
    nj, ni, nk, _ = d_ref.shape

    def sides(dim, length, step=1):
        count, halo = counts[dim], halos[dim]
        face = faces[dim] if emit else (None,) * len(halo)
        if count == 2:
            upper = lax.axis_index(AXES[dim]) == 0
            return [(jnp.where(upper, length - step, 0), jnp.where(upper, -1.0, 1.0), halo[0], face[0])]
        if count > 2:
            return [(0, 1.0, halo[0], face[0]), (length - step, -1.0, halo[1], face[1])]
        return []

    tile = 8
    row = lax.broadcasted_iota(jnp.int32, (tile, d_ref.shape[3]), 0)
    for start, sign, halo, _ in sides(2, nk, tile):
        start = pl.multiple_of(start, tile) if not isinstance(start, int) else start
        own = jnp.where(sign > 0, 0, tile - 1) if not isinstance(sign, float) else (0 if sign > 0 else tile - 1)
        mask = jnp.where(row == own, 1.0, 0.0)
        for j in range(nj):

            @pl.loop(0, ni, unroll=8)
            def _(i, j=j):
                weight = (RATE + sign * fk_ref[j, i, pl.ds(start, tile)]) * mask
                o_ref[j, i, pl.ds(start, tile)] = d_ref[j, i, pl.ds(start, tile)] + weight * halo[j, pl.ds(i, 1)]

    for at_i, sign, halo, _ in sides(1, ni):
        for j in range(nj):
            o_ref[j, at_i] = o_ref[j, at_i] + (RATE + sign * fi_ref[j, at_i]) * halo[j]
    for at_j, sign, halo, face in sides(0, nj):

        @pl.loop(0, ni)
        def _(i, at_j=at_j, sign=sign, halo=halo, face=face):
            out = o_ref[at_j, i] + (RATE + sign * fj_ref[at_j, i]) * halo[i]
            o_ref[at_j, i] = out

    if emit:
        for dim, length in ((0, nj), (1, ni), (2, nk)):
            for at_d, _, _, face in sides(dim, length):
                if dim == 0:

                    @pl.loop(0, ni)
                    def _(i, at_d=at_d, face=face):
                        face[i] = o_ref[at_d, i]

                elif dim == 1:
                    for j in range(nj):
                        face[j] = o_ref[j, at_d]
                else:
                    for j in range(nj):

                        @pl.loop(0, ni, unroll=8)
                        def _(i, j=j, at_d=at_d, face=face):
                            face[j, pl.ds(i, 1)] = o_ref[j, i, pl.ds(at_d, 1)]


VM = pl.BlockSpec(memory_space=pltpu.VMEM)


def per_device(density, flow_j, flow_i, flow_k):
    counts = [lax.axis_size(axis) for axis in AXES]
    shape, dtype = density.shape, density.dtype
    cells = density.size
    face_shapes = [shape[:d] + shape[d + 1 :] for d in range(3)]
    flows = (flow_j, flow_i, flow_k)
    limit = 24 * 2**20

    def first_faces(x):
        out = []
        for dim, (axis, count) in enumerate(zip(AXES, counts)):
            n = shape[dim]
            if count == 2:
                start = jnp.where(lax.axis_index(axis) == 0, n - 1, 0)
                out.append([lax.dynamic_index_in_dim(x, start, dim, keepdims=False)])
            elif count > 2:
                out.append([lax.index_in_dim(x, at, dim, keepdims=False) for at in (0, n - 1)])
            else:
                out.append([])
        return out

    def swap_order(faces):
        halos = [None] * 3
        for dim in (1, 0, 2):
            halos[dim] = exchange(AXES[dim], faces[dim]) if faces[dim] else []
        return halos

    main = pl.pallas_call(
        main_kernel,
        out_shape=pltpu.VMEM(shape, dtype),
        in_specs=[VM] * 4,
        out_specs=VM,
        name="main",
        compiler_params=pltpu.CompilerParams(vmem_limit_bytes=limit),
        cost_estimate=pl.CostEstimate(flops=24 * cells, bytes_accessed=20 * cells, transcendentals=0),
    )

    def patch(x, halos, emit):
        flat = [h for hs in halos for h in hs]
        outs = [pltpu.VMEM(shape, dtype)]
        if emit:
            outs += [pltpu.VMEM(face_shapes[d], dtype) for d in range(3) for _ in halos[d]]
        got = pl.pallas_call(
            functools.partial(patch_kernel, counts, emit),
            out_shape=outs,
            in_specs=[VM] * (4 + len(flat)),
            out_specs=[VM] * len(outs),
            input_output_aliases={0: 0},
            name="patch",
            compiler_params=pltpu.CompilerParams(vmem_limit_bytes=limit),
            cost_estimate=pl.CostEstimate(flops=cells, bytes_accessed=cells, transcendentals=0),
        )(x, *flows, *flat)
        x, rest, faces = got[0], list(got[1:]), []
        for d in range(3):
            size = len(halos[d]) if emit else 0
            faces.append(rest[:size])
            rest = rest[size:]
        return x, faces

    faces = first_faces(density)
    for step in range(STEPS):
        halos = swap_order(faces)
        density = main(density, *flows)
        density, faces = patch(density, halos, step < STEPS - 1)
    return density


def solution(mesh):
    spec = P(("ens", "south"), "east", "down", None)
    return jax.shard_map(per_device, mesh=mesh, in_specs=(spec,) * 4, out_specs=spec, check_vma=False)
```

```python
import functools

import jax
import jax.numpy as jnp
from jax import lax
from jax.experimental import pallas as pl
from jax.experimental.pallas import tpu as pltpu
from jax.sharding import PartitionSpec as P

STEPS = 3
AXES = ("south", "east", "down")
RATE = 0.05
PIECES = 8


def rounds(count):
    return [[(i, i + 1) for i in range(begin, count - 1, 2)] for begin in range(min(2, count - 1))]


def exchange(axis, faces):
    pairs = rounds(lax.axis_size(axis))
    return [lax.ppermute(face, axis, up + [(j, i) for i, j in up]) for face, up in zip(faces, pairs)]


def sides(dim, count, length, step=1):
    out = []
    for begin in range(len(rounds(count))):
        upper = lax.axis_index(AXES[dim]) % 2 == begin
        out.append((jnp.where(upper, length - step, 0), jnp.where(upper, -1.0, 1.0)))
    return out


def copy_faces(counts, o_ref, faces, planes=None):
    nj, ni, nk, _ = o_ref.shape
    for j in range(nj) if planes is None else planes:
        for (at, _), face in zip(sides(1, counts[1], ni), faces[1]):
            face[j] = o_ref[j, at]
        for (at, _), face in zip(sides(2, counts[2], nk), faces[2]):

            @pl.loop(0, ni, unroll=8)
            def _(i, j=j, at=at, face=face):
                face[j, pl.ds(i, 1)] = o_ref[j, i, pl.ds(at, 1)]


def copy_face_j(counts, o_ref, faces):
    for (at, _), face in zip(sides(0, counts[0], o_ref.shape[0]), faces[0]):

        @pl.loop(0, o_ref.shape[1], unroll=2)
        def _(i, at=at, face=face):
            face[i] = o_ref[at, i]


def grouped(refs, counts):
    out, at = [], 0
    for count in counts:
        size = len(rounds(count))
        out.append(refs[at : at + size])
        at += size
    return out


def load_kernel(counts, x_ref, *refs):
    d_ref, sems = refs[0], refs[-1]
    faces = grouped(refs[1:-1], counts)
    copies = [pltpu.make_async_copy(x_ref.at[j], d_ref.at[j], sems.at[j]) for j in range(d_ref.shape[0])]
    for copy in copies:
        copy.start()
    for j, copy in enumerate(copies):
        copy.wait()
        copy_faces(counts, d_ref, faces, [j])
    copy_face_j(counts, d_ref, faces)


def update(d_ref, flow_refs, o_ref, i, below, above):
    fj_ref, fi_ref, fk_ref = flow_refs
    nj, _, nk, lanes = d_ref.shape
    tile = 8
    row = lax.broadcasted_iota(jnp.int32, (tile, lanes), 0)
    own = [d_ref[j, i] for j in range(nj)]

    def terms(flow, lower, upper):
        if lower is None and upper is None:
            return None
        if lower is None:
            return upper, -(flow * upper)
        if upper is None:
            return lower, flow * lower
        return lower + upper, flow * (lower - upper)

    for j in range(nj):
        m = own[j]
        km = pltpu.roll(m, 1, 0)
        kp = pltpu.roll(m, nk - 1, 0)
        km = jnp.concatenate([jnp.where(row == 0, 0.0, km[:tile]), km[tile:]], 0)
        kp = jnp.concatenate([kp[: nk - tile], jnp.where(row == tile - 1, 0.0, kp[nk - tile :])], 0)
        parts = [
            terms(fk_ref[j, i], km, kp),
            terms(fi_ref[j, i], None if below is None else d_ref[j, below], None if above is None else d_ref[j, above]),
            terms(fj_ref[j, i], own[j - 1] if j > 0 else None, own[j + 1] if j < nj - 1 else None),
        ]
        parts = [part for part in parts if part is not None]
        total = functools.reduce(jnp.add, [part[0] for part in parts])
        drift = functools.reduce(jnp.add, [part[1] for part in parts])
        o_ref[j, i] = (1.0 - 6.0 * RATE) * m + drift + RATE * total


def update_rows(d_ref, flow_refs, o_ref, start, stop):
    ni = d_ref.shape[1]
    if start == 0:
        update(d_ref, flow_refs, o_ref, 0, None, 1 if ni > 1 else None)
    lo, hi = max(start, 1), min(stop, ni - 1)
    if hi > lo:

        @pl.loop(lo, hi)
        def _(i):
            update(d_ref, flow_refs, o_ref, i, i - 1, i + 1)

    if stop == ni and ni > 1:
        update(d_ref, flow_refs, o_ref, ni - 1, ni - 2, None)


def main_kernel(d_ref, fj_ref, fi_ref, fk_ref, o_ref):
    update_rows(d_ref, (fj_ref, fi_ref, fk_ref), o_ref, 0, d_ref.shape[1])


def first_kernel(d_ref, fj_hbm, fi_hbm, fk_hbm, o_ref, fj_ref, fi_ref, fk_ref, sems):
    ni = d_ref.shape[1]
    pieces = sems.shape[1]
    rows = ni // pieces
    flow_refs = (fj_ref, fi_ref, fk_ref)

    def copy(n, piece):
        at = pl.ds(piece * rows, rows)
        hbm = (fj_hbm, fi_hbm, fk_hbm)[n]
        return pltpu.make_async_copy(hbm.at[:, at], flow_refs[n].at[:, at], sems.at[n, piece])

    for piece in range(pieces):
        for n in range(3):
            copy(n, piece).start()
    for piece in range(pieces):
        for n in range(3):
            copy(n, piece).wait()
        update_rows(d_ref, flow_refs, o_ref, piece * rows, (piece + 1) * rows)


def patch_kernel(counts, emit, *refs):
    d_ref, fj_ref, fi_ref, fk_ref = refs[:4]
    size = sum(len(rounds(count)) for count in counts)
    halos = grouped(refs[4 : 4 + size], counts)
    o_ref = refs[4 + size]
    nj, ni, nk, _ = d_ref.shape
    tile = 8
    row = lax.broadcasted_iota(jnp.int32, (tile, d_ref.shape[3]), 0)
    for (start, sign), halo in zip(sides(2, counts[2], nk, tile), halos[2]):
        start = pl.multiple_of(start, tile)
        mask = jnp.where(row == jnp.where(sign > 0, 0, tile - 1), 1.0, 0.0)
        for j in range(nj):

            @pl.loop(0, ni, unroll=8)
            def _(i, j=j, start=start, sign=sign, mask=mask, halo=halo):
                weight = (RATE + sign * fk_ref[j, i, pl.ds(start, tile)]) * mask
                o_ref[j, i, pl.ds(start, tile)] = d_ref[j, i, pl.ds(start, tile)] + weight * halo[j, pl.ds(i, 1)]

    for (at, sign), halo in zip(sides(1, counts[1], ni), halos[1]):
        for j in range(nj):
            o_ref[j, at] = o_ref[j, at] + (RATE + sign * fi_ref[j, at]) * halo[j]
    for (at, sign), halo in zip(sides(0, counts[0], nj), halos[0]):

        @pl.loop(0, ni, unroll=2)
        def _(i, at=at, sign=sign, halo=halo):
            o_ref[at, i] = o_ref[at, i] + (RATE + sign * fj_ref[at, i]) * halo[i]

    if emit:
        faces = grouped(refs[5 + size :], counts)
        copy_face_j(counts, o_ref, faces)
        copy_faces(counts, o_ref, faces)


VM = pl.BlockSpec(memory_space=pltpu.VMEM)
HBM = pl.BlockSpec(memory_space=pltpu.HBM)


def per_device(density, *flows):
    counts = [lax.axis_size(axis) for axis in AXES]
    shape, dtype = density.shape, density.dtype
    cells = density.size
    whole = pltpu.VMEM(shape, dtype)
    faces_out = [
        pltpu.VMEM(shape[:d] + shape[d + 1 :], dtype) for d in range(3) for _ in rounds(counts[d])
    ]
    params = pltpu.CompilerParams(vmem_limit_bytes=24 * 2**20)

    def cost(flops, moved):
        return pl.CostEstimate(flops=flops * cells, bytes_accessed=moved * cells, transcendentals=0)

    def patch(x, halos, emit):
        flat = [h for hs in halos for h in hs]
        outs = [whole] + (faces_out if emit else [])
        got = pl.pallas_call(
            functools.partial(patch_kernel, counts, emit),
            out_shape=outs,
            in_specs=[VM] * (4 + len(flat)),
            out_specs=[VM] * len(outs),
            input_output_aliases={0: 0},
            name="patch",
            compiler_params=params,
            cost_estimate=cost(1, 1),
        )(x, *flows, *flat)
        return got[0], list(got[1:])

    density, *faces = pl.pallas_call(
        functools.partial(load_kernel, counts),
        out_shape=[whole] + faces_out,
        in_specs=[HBM],
        out_specs=[VM] * (1 + len(faces_out)),
        scratch_shapes=[pltpu.SemaphoreType.DMA((shape[0],))],
        name="load",
        compiler_params=params,
        cost_estimate=cost(1, 4),
    )(density)
    for step in range(STEPS):
        groups = grouped(faces, counts)
        halos = [None] * 3
        for dim in (1, 0, 2):
            halos[dim] = exchange(AXES[dim], groups[dim])
        if step == 0:
            density, *flows = pl.pallas_call(
                first_kernel,
                out_shape=[whole] * 4,
                in_specs=[VM] + [HBM] * 3,
                out_specs=[VM] * 4,
                scratch_shapes=[pltpu.SemaphoreType.DMA((3, PIECES if shape[1] % PIECES == 0 else 1))],
                name="first",
                compiler_params=params,
                cost_estimate=cost(24, 20),
            )(density, *flows)
        else:
            density = pl.pallas_call(
                main_kernel,
                out_shape=whole,
                in_specs=[VM] * 4,
                out_specs=VM,
                name="main",
                compiler_params=params,
                cost_estimate=cost(24, 20),
            )(density, *flows)
        density, faces = patch(density, halos, step < STEPS - 1)
    return density


def solution(mesh):
    spec = P(("ens", "south"), "east", "down", None)
    return jax.shard_map(per_device, mesh=mesh, in_specs=(spec,) * 4, out_specs=spec, check_vma=False)
```

```python
import functools

import jax
import jax.numpy as jnp
from jax import lax
from jax.experimental import pallas as pl
from jax.experimental.pallas import tpu as pltpu
from jax.sharding import PartitionSpec as P


STEPS = 3
AXES = ("south", "east", "down")
RATE = 0.05
PIECES = 8
ORDER = (1, 0, 2)


def rounds(count):
    return [[(i, i + 1) for i in range(begin, count - 1, 2)] for begin in range(min(2, count - 1))]


def exchange_all(groups, counts):
    halos = [[] for _ in AXES]
    for dim in ORDER:
        for face, up in zip(groups[dim], rounds(counts[dim])):
            halos[dim].append(lax.ppermute(face, AXES[dim], up + [(j, i) for i, j in up]))
    return halos


def sides(dim, count, length, step=1):
    out = []
    for begin in range(len(rounds(count))):
        upper = lax.axis_index(AXES[dim]) % 2 == begin
        out.append((jnp.where(upper, length - step, 0), jnp.where(upper, -1.0, 1.0)))
    return out


def copy_faces(counts, o_ref, faces, planes=None):
    nj, ni, nk, _ = o_ref.shape
    for j in range(nj) if planes is None else planes:
        for (at, _), face in zip(sides(1, counts[1], ni), faces[1]):
            face[j] = o_ref[j, at]
        for (at, _), face in zip(sides(2, counts[2], nk), faces[2]):

            @pl.loop(0, ni, unroll=8)
            def _(i, j=j, at=at, face=face):
                face[j, pl.ds(i, 1)] = o_ref[j, i, pl.ds(at, 1)]


def copy_face_j(counts, o_ref, faces):
    for (at, _), face in zip(sides(0, counts[0], o_ref.shape[0]), faces[0]):

        @pl.loop(0, o_ref.shape[1], unroll=2)
        def _(i, at=at, face=face):
            face[i] = o_ref[at, i]


def grouped(refs, counts):
    out, at = [], 0
    for count in counts:
        size = len(rounds(count))
        out.append(refs[at : at + size])
        at += size
    return out


def load_kernel(counts, x_ref, *refs):
    d_ref, sems = refs[0], refs[-1]
    faces = grouped(refs[1:-1], counts)
    copies = [pltpu.make_async_copy(x_ref.at[j], d_ref.at[j], sems.at[j]) for j in range(d_ref.shape[0])]
    for copy in copies:
        copy.start()
    for j, copy in enumerate(copies):
        copy.wait()
        copy_faces(counts, d_ref, faces, [j])
    copy_face_j(counts, d_ref, faces)


def update(d_ref, flow_refs, o_ref, i, below, above):
    fj_ref, fi_ref, fk_ref = flow_refs
    nj, _, nk, lanes = d_ref.shape
    tile = 8
    row = lax.broadcasted_iota(jnp.int32, (tile, lanes), 0)
    own = [d_ref[j, i] for j in range(nj)]

    def terms(flow, lower, upper):
        if lower is None and upper is None:
            return None
        if lower is None:
            return upper, -(flow * upper)
        if upper is None:
            return lower, flow * lower
        return lower + upper, flow * (lower - upper)

    for j in range(nj):
        m = own[j]
        km = pltpu.roll(m, 1, 0)
        kp = pltpu.roll(m, nk - 1, 0)
        km = jnp.concatenate([jnp.where(row == 0, 0.0, km[:tile]), km[tile:]], 0)
        kp = jnp.concatenate([kp[: nk - tile], jnp.where(row == tile - 1, 0.0, kp[nk - tile :])], 0)
        parts = [
            terms(fk_ref[j, i], km, kp),
            terms(fi_ref[j, i], None if below is None else d_ref[j, below], None if above is None else d_ref[j, above]),
            terms(fj_ref[j, i], own[j - 1] if j > 0 else None, own[j + 1] if j < nj - 1 else None),
        ]
        parts = [part for part in parts if part is not None]
        total = functools.reduce(jnp.add, [part[0] for part in parts])
        drift = functools.reduce(jnp.add, [part[1] for part in parts])
        o_ref[j, i] = (1.0 - 6.0 * RATE) * m + drift + RATE * total


def update_rows(d_ref, flow_refs, o_ref, start, stop):
    ni = d_ref.shape[1]
    if start == 0:
        update(d_ref, flow_refs, o_ref, 0, None, 1 if ni > 1 else None)
    lo, hi = max(start, 1), min(stop, ni - 1)
    if hi > lo:

        @pl.loop(lo, hi)
        def _(i):
            update(d_ref, flow_refs, o_ref, i, i - 1, i + 1)

    if stop == ni and ni > 1:
        update(d_ref, flow_refs, o_ref, ni - 1, ni - 2, None)


def main_kernel(start, stop, d_ref, fj_ref, fi_ref, fk_ref, *refs):
    update_rows(d_ref, (fj_ref, fi_ref, fk_ref), refs[-1], start, stop)


def first_kernel(d_ref, fj_hbm, fi_hbm, fk_hbm, o_ref, fj_ref, fi_ref, fk_ref, sems):
    ni = d_ref.shape[1]
    pieces = sems.shape[1]
    rows = ni // pieces
    flow_refs = (fj_ref, fi_ref, fk_ref)

    def copy(n, piece):
        at = pl.ds(piece * rows, rows)
        hbm = (fj_hbm, fi_hbm, fk_hbm)[n]
        return pltpu.make_async_copy(hbm.at[:, at], flow_refs[n].at[:, at], sems.at[n, piece])

    for piece in range(pieces):
        for n in range(3):
            copy(n, piece).start()
    for piece in range(pieces):
        for n in range(3):
            copy(n, piece).wait()
        update_rows(d_ref, flow_refs, o_ref, piece * rows, (piece + 1) * rows)


def patch_kernel(counts, emit, *refs):
    d_ref, fj_ref, fi_ref, fk_ref = refs[:4]
    size = sum(len(rounds(count)) for count in counts)
    halos = grouped(refs[4 : 4 + size], counts)
    o_ref = refs[4 + size]
    nj, ni, nk, _ = d_ref.shape
    tile = 8
    row = lax.broadcasted_iota(jnp.int32, (tile, d_ref.shape[3]), 0)
    for (start, sign), halo in zip(sides(2, counts[2], nk, tile), halos[2]):
        start = pl.multiple_of(start, tile)
        mask = jnp.where(row == jnp.where(sign > 0, 0, tile - 1), 1.0, 0.0)
        for j in range(nj):

            @pl.loop(0, ni, unroll=8)
            def _(i, j=j, start=start, sign=sign, mask=mask, halo=halo):
                weight = (RATE + sign * fk_ref[j, i, pl.ds(start, tile)]) * mask
                o_ref[j, i, pl.ds(start, tile)] = d_ref[j, i, pl.ds(start, tile)] + weight * halo[j, pl.ds(i, 1)]

    for (at, sign), halo in zip(sides(1, counts[1], ni), halos[1]):
        for j in range(nj):
            o_ref[j, at] = o_ref[j, at] + (RATE + sign * fi_ref[j, at]) * halo[j]
    for (at, sign), halo in zip(sides(0, counts[0], nj), halos[0]):

        @pl.loop(0, ni, unroll=2)
        def _(i, at=at, sign=sign, halo=halo):
            o_ref[at, i] = o_ref[at, i] + (RATE + sign * fj_ref[at, i]) * halo[i]

    if emit:
        faces = grouped(refs[5 + size :], counts)
        copy_face_j(counts, o_ref, faces)
        copy_faces(counts, o_ref, faces)


VM = pl.BlockSpec(memory_space=pltpu.VMEM)
HBM = pl.BlockSpec(memory_space=pltpu.HBM)


def per_device(density, *flows):
    counts = [lax.axis_size(axis) for axis in AXES]
    shape, dtype = density.shape, density.dtype
    cells = density.size
    whole = pltpu.VMEM(shape, dtype)
    faces_out = [
        pltpu.VMEM(shape[:d] + shape[d + 1 :], dtype) for d in range(3) for _ in rounds(counts[d])
    ]
    params = pltpu.CompilerParams(vmem_limit_bytes=24 * 2**20)

    def cost(flops, moved):
        return pl.CostEstimate(flops=flops * cells, bytes_accessed=moved * cells, transcendentals=0)

    def patch(x, halos, emit):
        flat = [h for hs in halos for h in hs]
        outs = [whole] + (faces_out if emit else [])
        got = pl.pallas_call(
            functools.partial(patch_kernel, counts, emit),
            out_shape=outs,
            in_specs=[VM] * (4 + len(flat)),
            out_specs=[VM] * len(outs),
            input_output_aliases={0: 0},
            name="patch",
            compiler_params=params,
            cost_estimate=cost(1, 1),
        )(x, *flows, *flat)
        return got[0], list(got[1:])

    density, *faces = pl.pallas_call(
        functools.partial(load_kernel, counts),
        out_shape=[whole] + faces_out,
        in_specs=[HBM],
        out_specs=[VM] * (1 + len(faces_out)),
        scratch_shapes=[pltpu.SemaphoreType.DMA((shape[0],))],
        name="load",
        compiler_params=params,
        cost_estimate=cost(1, 4),
    )(density)
    messages = len(faces_out)
    for step in range(STEPS):
        halos = exchange_all(grouped(faces, counts), counts)
        if step == 0:
            density, *flows = pl.pallas_call(
                first_kernel,
                out_shape=[whole] * 4,
                in_specs=[VM] + [HBM] * 3,
                out_specs=[VM] * 4,
                scratch_shapes=[pltpu.SemaphoreType.DMA((3, PIECES if shape[1] % PIECES == 0 else 1))],
                name="first",
                compiler_params=params,
                cost_estimate=cost(24, 20),
            )(density, *flows)
        else:
            parts = max(1, min(messages, shape[1]))
            done = []
            for part in range(parts):
                start, stop = (shape[1] * at // parts for at in (part, part + 1))
                done = [
                    pl.pallas_call(
                        functools.partial(main_kernel, start, stop),
                        out_shape=whole,
                        in_specs=[VM] * (4 + len(done)),
                        out_specs=VM,
                        input_output_aliases={4: 0} if done else {},
                        name="main",
                        compiler_params=params,
                        cost_estimate=cost(24 // parts, 20 // parts),
                    )(density, *flows, *done)
                ]
            density = done[0]
        density, faces = patch(density, halos, step < STEPS - 1)
    return density


def solution(mesh):
    spec = P(("ens", "south"), "east", "down", None)
    return jax.shard_map(per_device, mesh=mesh, in_specs=(spec,) * 4, out_specs=spec, check_vma=False)
```

```python
import functools

import jax
import jax.numpy as jnp
from jax import lax
from jax.experimental import pallas as pl
from jax.experimental.pallas import tpu as pltpu
from jax.sharding import PartitionSpec as P

STEPS = 3
AXES = ("south", "east", "down")
RATE = 0.05
PIECES = 8


def rounds(count):
    return [[(i, i + 1) for i in range(begin, count - 1, 2)] for begin in range(min(2, count - 1))]


def exchange(axis, faces):
    pairs = rounds(lax.axis_size(axis))
    return [lax.ppermute(face, axis, up + [(j, i) for i, j in up]) for face, up in zip(faces, pairs)]


def sides(dim, count, length, step=1):
    out = []
    for begin in range(len(rounds(count))):
        upper = lax.axis_index(AXES[dim]) % 2 == begin
        out.append((jnp.where(upper, length - step, 0), jnp.where(upper, -1.0, 1.0)))
    return out


def copy_faces(counts, o_ref, faces, planes=None):
    nj, ni, nk, _ = o_ref.shape
    for j in range(nj) if planes is None else planes:
        for (at, _), face in zip(sides(1, counts[1], ni), faces[1]):
            face[j] = o_ref[j, at]
        for (at, _), face in zip(sides(2, counts[2], nk), faces[2]):

            @pl.loop(0, ni, unroll=8)
            def _(i, j=j, at=at, face=face):
                face[j, pl.ds(i, 1)] = o_ref[j, i, pl.ds(at, 1)]


def copy_face_j(counts, o_ref, faces):
    for (at, _), face in zip(sides(0, counts[0], o_ref.shape[0]), faces[0]):

        @pl.loop(0, o_ref.shape[1], unroll=2)
        def _(i, at=at, face=face):
            face[i] = o_ref[at, i]


def grouped(refs, counts):
    out, at = [], 0
    for count in counts:
        size = len(rounds(count))
        out.append(refs[at : at + size])
        at += size
    return out


def load_kernel(counts, x_ref, *refs):
    d_ref, sems = refs[0], refs[-1]
    faces = grouped(refs[1:-1], counts)
    copies = [pltpu.make_async_copy(x_ref.at[j], d_ref.at[j], sems.at[j]) for j in range(d_ref.shape[0])]
    for copy in copies:
        copy.start()
    for j, copy in enumerate(copies):
        copy.wait()
        copy_faces(counts, d_ref, faces, [j])
    copy_face_j(counts, d_ref, faces)


def update(d_ref, flow_refs, o_ref, i, below, above):
    fj_ref, fi_ref, fk_ref = flow_refs
    nj, _, nk, lanes = d_ref.shape
    tile = 8
    row = lax.broadcasted_iota(jnp.int32, (tile, lanes), 0)
    own = [d_ref[j, i] for j in range(nj)]

    def terms(flow, lower, upper):
        if lower is None and upper is None:
            return None
        if lower is None:
            return upper, -(flow * upper)
        if upper is None:
            return lower, flow * lower
        return lower + upper, flow * (lower - upper)

    for j in range(nj):
        m = own[j]
        km = pltpu.roll(m, 1, 0)
        kp = pltpu.roll(m, nk - 1, 0)
        km = jnp.concatenate([jnp.where(row == 0, 0.0, km[:tile]), km[tile:]], 0)
        kp = jnp.concatenate([kp[: nk - tile], jnp.where(row == tile - 1, 0.0, kp[nk - tile :])], 0)
        parts = [
            terms(fk_ref[j, i], km, kp),
            terms(fi_ref[j, i], None if below is None else d_ref[j, below], None if above is None else d_ref[j, above]),
            terms(fj_ref[j, i], own[j - 1] if j > 0 else None, own[j + 1] if j < nj - 1 else None),
        ]
        parts = [part for part in parts if part is not None]
        total = functools.reduce(jnp.add, [part[0] for part in parts])
        drift = functools.reduce(jnp.add, [part[1] for part in parts])
        o_ref[j, i] = (1.0 - 6.0 * RATE) * m + drift + RATE * total


def update_rows(d_ref, flow_refs, o_ref, start, stop):
    ni = d_ref.shape[1]
    if start == 0:
        update(d_ref, flow_refs, o_ref, 0, None, 1 if ni > 1 else None)
    lo, hi = max(start, 1), min(stop, ni - 1)
    if hi > lo:

        @pl.loop(lo, hi)
        def _(i):
            update(d_ref, flow_refs, o_ref, i, i - 1, i + 1)

    if stop == ni and ni > 1:
        update(d_ref, flow_refs, o_ref, ni - 1, ni - 2, None)


def main_kernel(d_ref, fj_ref, fi_ref, fk_ref, o_ref):
    update_rows(d_ref, (fj_ref, fi_ref, fk_ref), o_ref, 0, d_ref.shape[1])


def first_kernel(d_ref, fj_hbm, fi_hbm, fk_hbm, o_ref, fj_ref, fi_ref, fk_ref, sems):
    ni = d_ref.shape[1]
    pieces = sems.shape[1]
    rows = ni // pieces
    flow_refs = (fj_ref, fi_ref, fk_ref)

    def copy(n, piece):
        at = pl.ds(piece * rows, rows)
        hbm = (fj_hbm, fi_hbm, fk_hbm)[n]
        return pltpu.make_async_copy(hbm.at[:, at], flow_refs[n].at[:, at], sems.at[n, piece])

    for piece in range(pieces):
        for n in range(3):
            copy(n, piece).start()
    for piece in range(pieces):
        for n in range(3):
            copy(n, piece).wait()
        update_rows(d_ref, flow_refs, o_ref, piece * rows, (piece + 1) * rows)


def patch_kernel(counts, emit, *refs):
    d_ref, fj_ref, fi_ref, fk_ref = refs[:4]
    size = sum(len(rounds(count)) for count in counts)
    halos = grouped(refs[4 : 4 + size], counts)
    o_ref = refs[4 + size]
    nj, ni, nk, _ = d_ref.shape
    tile = 8
    row = lax.broadcasted_iota(jnp.int32, (tile, d_ref.shape[3]), 0)
    rows_k = []
    for (start, sign), halo in zip(sides(2, counts[2], nk, tile), halos[2]):
        start = pl.multiple_of(start, tile)
        mask = jnp.where(row == jnp.where(sign > 0, 0, tile - 1), 1.0, 0.0)
        rows_k.append((start, sign, mask, halo))

    def plane(j):
        for start, sign, mask, halo in rows_k:

            @pl.loop(0, ni, unroll=8)
            def _(i, start=start, sign=sign, mask=mask, halo=halo):
                weight = (RATE + sign * fk_ref[j, i, pl.ds(start, tile)]) * mask
                o_ref[j, i, pl.ds(start, tile)] = d_ref[j, i, pl.ds(start, tile)] + weight * halo[j, pl.ds(i, 1)]

        for (at, sign), halo in zip(sides(1, counts[1], ni), halos[1]):
            o_ref[j, at] = o_ref[j, at] + (RATE + sign * fi_ref[j, at]) * halo[j]
    outer = sides(0, counts[0], nj)
    order = [lax.rem(outer[0][0] + n, nj) for n in range(1, nj + 1)] if len(outer) == 1 else list(range(nj))
    early = nj - 1 if len(outer) == 1 else 0 if outer else nj
    copies = []

    def send(n):
        if not emit:
            copies.append(pltpu.make_async_copy(o_ref.at[order[n]], refs[5 + size].at[order[n]], refs[-1].at[n]))
            copies[-1].start()

    for n in range(nj):
        plane(order[n])
        if n < early:
            send(n)
    for (at, sign), halo in zip(outer, halos[0]):

        @pl.loop(0, ni, unroll=2)
        def _(i, at=at, sign=sign, halo=halo):
            o_ref[at, i] = o_ref[at, i] + (RATE + sign * fj_ref[at, i]) * halo[i]

    for n in range(early, nj):
        send(n)
    for copy in copies:
        copy.wait()
    if emit:
        faces = grouped(refs[5 + size :], counts)
        copy_face_j(counts, o_ref, faces)
        copy_faces(counts, o_ref, faces)


VM = pl.BlockSpec(memory_space=pltpu.VMEM)
HBM = pl.BlockSpec(memory_space=pltpu.HBM)


def per_device(density, *flows):
    counts = [lax.axis_size(axis) for axis in AXES]
    shape, dtype = density.shape, density.dtype
    cells = density.size
    whole = pltpu.VMEM(shape, dtype)
    faces_out = [
        pltpu.VMEM(shape[:d] + shape[d + 1 :], dtype) for d in range(3) for _ in rounds(counts[d])
    ]
    params = pltpu.CompilerParams(vmem_limit_bytes=24 * 2**20)

    def cost(flops, moved):
        return pl.CostEstimate(flops=flops * cells, bytes_accessed=moved * cells, transcendentals=0)

    def patch(x, halos, emit):
        flat = [h for hs in halos for h in hs]
        outs = [whole] + (faces_out if emit else [pltpu.HBM(shape, dtype)])
        got = pl.pallas_call(
            functools.partial(patch_kernel, counts, emit),
            out_shape=outs,
            in_specs=[VM] * (4 + len(flat)),
            out_specs=[VM] * len(outs) if emit else [VM, HBM],
            input_output_aliases={0: 0},
            scratch_shapes=[] if emit else [pltpu.SemaphoreType.DMA((shape[0],))],
            name="patch",
            compiler_params=params,
            cost_estimate=cost(1, 1),
        )(x, *flows, *flat)
        return got[0], list(got[1:])

    density, *faces = pl.pallas_call(
        functools.partial(load_kernel, counts),
        out_shape=[whole] + faces_out,
        in_specs=[HBM],
        out_specs=[VM] * (1 + len(faces_out)),
        scratch_shapes=[pltpu.SemaphoreType.DMA((shape[0],))],
        name="load",
        compiler_params=params,
        cost_estimate=cost(1, 4),
    )(density)
    for step in range(STEPS):
        groups = grouped(faces, counts)
        halos = [None] * 3
        for dim in (1, 0, 2):
            halos[dim] = exchange(AXES[dim], groups[dim])
        if step == 0:
            density, *flows = pl.pallas_call(
                first_kernel,
                out_shape=[whole] * 4,
                in_specs=[VM] + [HBM] * 3,
                out_specs=[VM] * 4,
                scratch_shapes=[pltpu.SemaphoreType.DMA((3, PIECES if shape[1] % PIECES == 0 else 1))],
                name="first",
                compiler_params=pltpu.CompilerParams(vmem_limit_bytes=28 * 2**20),
                cost_estimate=cost(24, 20),
            )(density, *flows)
        else:
            density = pl.pallas_call(
                main_kernel,
                out_shape=whole,
                in_specs=[VM] * 4,
                out_specs=VM,
                name="main",
                compiler_params=params,
                cost_estimate=cost(24, 20),
            )(density, *flows)
        density, faces = patch(density, halos, step < STEPS - 1)
    return faces[0]


def solution(mesh):
    spec = P(("ens", "south"), "east", "down", None)
    return jax.shard_map(per_device, mesh=mesh, in_specs=(spec,) * 4, out_specs=spec, check_vma=False)
```
